32 devices in a mesh: section: 8 (over y, x, core), ctx: 4 (over z).
Axes of the slice: x: 2, y: 2, z: 4, core: 2. Of those that a mesh axis runs over, the one named last changes fastest.
Arguments:
- section_inputs: bfloat16 [8, 448, 2048], P('section', 'ctx'), may hold values from -3 to 3
- saved_inputs: bfloat16 [8, 448, 2048], P('section', 'ctx'), may hold values from -3 to 3
- output_grads: bfloat16 [8, 448, 2048], P('section', 'ctx'), may hold values from -6 to 6
- token_positions: int32 [448], P('ctx'), may hold values from 0 to 447, each once
- norm_gain: float32 [8, 2048], P('section'), may hold values from 0.7 to 6
- query_weight: bfloat16 [8, 2048, 2048], P('section', 'ctx'), may hold values from -0.13258252 to 0.13258252
- keyval_weight: bfloat16 [8, 2048, 1024], P('section', 'ctx'), may hold values from -0.13258252 to 0.13258252
- output_weight: bfloat16 [8, 2048, 2048], P('section'), may hold values from -0.125 to 0.125
Outputs:
- next_inputs: bfloat16 [8, 448, 2048], P('section', 'ctx')
- input_grads: bfloat16 [8, 448, 2048], P('section', 'ctx')
The draws below stay inside these ranges and needn't reach their ends.
Inputs may be any that keep to these rules, and one draw needn't show every extreme that they name: `token_positions`: each position of the sequence once.
All inputs are finite; a program needn't handle non-finite values.
Results may differ from the reference program's by a relative error of at most 0.04.
The reference program's roundings to bfloat16 on the way (of `normed`, `rounded` and `mixed`) count: a program that leaves them out, or rounds other values in their place, can miss the bound.
Values may be sent and summed in bfloat16 or wider, within the bound.
A program may use at most 192 MiB of HBM per device.

```python
import jax
import jax.numpy as jnp
from jax import lax

D = 2048
HEADS = 16
KV_HEADS = 4
HEAD_DIM = 128
SECTIONS = 8
SEQ = 448


def paired_weights(key):
    query_key = jax.random.fold_in(key, 11)
    keyval_key = jax.random.fold_in(key, 12)
    query_matrix = jax.random.truncated_normal(query_key, -4.0, 4.0, (SECTIONS, D, HEADS * HEAD_DIM), jnp.float32) * D ** (-0.5)
    keyval_matrix = jax.random.truncated_normal(keyval_key, -4.0, 4.0, (SECTIONS, D, 2 * KV_HEADS * HEAD_DIM), jnp.float32) * D ** (-0.5)
    return (query_matrix, keyval_matrix)


def draw_query_weight(key, part):
    return paired_weights(key)[0].astype(jnp.bfloat16)


def draw_keyval_weight(key, part):
    return paired_weights(key)[1].astype(jnp.bfloat16)


def draw_norm_gain(key, part):
    gain_key = jax.random.fold_in(key, 21)
    return 1.0 + 0.1 * jax.random.truncated_normal(gain_key, -3.0, 3.0, (SECTIONS, D), jnp.float32)


def block_levels(key, dims, shards, low, top_value):
    level, own = 1.0, jax.random.fold_in(key, 6)
    for axis_at, shards_of in shards:
        steps = jnp.exp(jax.random.uniform(jax.random.fold_in(own, axis_at), (shards_of,), jnp.float32, low / len(shards), top_value / len(shards)))
        level = level * jnp.repeat(steps, dims[axis_at] // shards_of).reshape([-1 if axis == axis_at else 1 for axis in range(len(dims))])
    return level


def normal_values(key, shape, spread, bound, cuts=(), kind=jnp.bfloat16):
    array = spread * jax.random.normal(key, shape, jnp.float32)
    if cuts:
        array = array * block_levels(key, shape, cuts, -0.22, 0.18)
    return jnp.clip(array, -bound, bound).astype(kind)


def setup_inputs(seed: int = 0) -> dict:
    keys = jax.random.split(jax.random.key(seed), 9)
    section_inputs = normal_values(keys[0], (SECTIONS, SEQ, D), 0.5, 3.0, ((0, 8), (1, 4)))
    saved_inputs = normal_values(keys[1], (SECTIONS, SEQ, D), 0.5, 3.0, ((0, 8), (1, 4)))
    output_grads = normal_values(keys[2], (SECTIONS, SEQ, D), 1.0, 6.0, ((0, 8), (1, 4)))
    token_positions = jax.random.permutation(keys[3], SEQ).astype(jnp.int32)
    norm_gain = draw_norm_gain(jax.random.fold_in(keys[8], 71), 0)
    query_weight = draw_query_weight(jax.random.fold_in(keys[8], 71), 0)
    keyval_weight = draw_keyval_weight(jax.random.fold_in(keys[8], 71), 0)
    output_weight = normal_values(keys[7], (SECTIONS, HEADS * HEAD_DIM, D), (HEADS * HEAD_DIM) ** -0.5, 0.125, ((0, 8),))
    return {"section_inputs": section_inputs, "saved_inputs": saved_inputs, "output_grads": output_grads, "token_positions": token_positions, "norm_gain": norm_gain, "query_weight": query_weight, "keyval_weight": keyval_weight, "output_weight": output_weight}


norm_eps = 1e-05
rope_base = 500000.0

def rotate(matrix, positions):
    half_dim = matrix.shape[-1] // 2
    frequency = rope_base ** (-2.0 * jnp.arange(half_dim, dtype=jnp.float32) / matrix.shape[-1])
    angles = positions.astype(jnp.float32)[:, None] * frequency[None, :]
    cos_table = jnp.cos(angles)[:, None, :]
    sin_table = jnp.sin(angles)[:, None, :]
    leading = matrix[..., :half_dim]
    trailing = matrix[..., half_dim:]
    return jnp.concatenate([leading * cos_table - trailing * sin_table, trailing * cos_table + leading * sin_table], axis=-1)

def project(tokens, gain, query_matrix, keyval_matrix, positions):
    widened = tokens.astype(jnp.float32)
    inverse = lax.rsqrt(lax.optimization_barrier(jnp.mean(widened * widened, axis=-1, keepdims=True)) + norm_eps)
    normed = (widened * inverse * gain[None, :]).astype(jnp.bfloat16)
    row_count = tokens.shape[0]
    query_full = jnp.dot(normed, query_matrix, preferred_element_type=jnp.float32)
    keyval_full = jnp.dot(normed, keyval_matrix, preferred_element_type=jnp.float32)
    queries = rotate(query_full.reshape(row_count, -1, HEAD_DIM), positions).astype(jnp.bfloat16)
    paired = keyval_full.reshape(row_count, 2, -1, HEAD_DIM)
    key_rows = rotate(paired[:, 0], positions).astype(jnp.bfloat16)
    value_rows = paired[:, 1].astype(jnp.bfloat16)
    return (queries, key_rows, value_rows)

def attend(queries, key_wide, value_wide, query_pos, key_pos):
    row_count = queries.shape[0]
    group_size = queries.shape[1] // key_wide.shape[1]
    grouped = queries.astype(jnp.float32).reshape(row_count, key_wide.shape[1], group_size, queries.shape[2])
    scores = jnp.einsum('rkgd,skd->kgrs', grouped, key_wide) * queries.shape[2] ** (-0.5)
    visible = (key_pos[None, :] <= query_pos[:, None])[None, None]
    masked = jnp.where(visible, scores, -1e+30)
    row_max = lax.stop_gradient(lax.optimization_barrier(jnp.max(masked, axis=-1, keepdims=True)))
    numerators = jnp.where(visible, jnp.exp(masked - row_max), 0.0)
    totals = lax.optimization_barrier(jnp.sum(numerators, axis=-1))
    rounded = lax.optimization_barrier(numerators.astype(jnp.bfloat16)).astype(jnp.float32)
    summed = jnp.einsum('kgrs,skd->rkgd', rounded, value_wide)
    averaged = summed / jnp.transpose(totals, (2, 0, 1))[..., None]
    return averaged.reshape(row_count, -1).astype(jnp.bfloat16)

def finish(tokens, mixed, output_matrix):
    return (tokens.astype(jnp.float32) + jnp.dot(mixed, output_matrix, preferred_element_type=jnp.float32)).astype(jnp.bfloat16)

def section_layer(tokens, gain, query_matrix, keyval_matrix, output_matrix, positions):
    queries, key_rows, value_rows = project(tokens, gain, query_matrix, keyval_matrix, positions)
    mixed = attend(queries, key_rows.astype(jnp.float32), value_rows.astype(jnp.float32), positions, positions)
    return finish(tokens, mixed, output_matrix)

def reference(section_inputs, saved_inputs, output_grads, token_positions, norm_gain, query_weight, keyval_weight, output_weight):

    def one_section(packed):
        forward_tokens, saved_tokens, upstream, gain, query_matrix, keyval_matrix, output_matrix = packed

        def layer(tokens):
            return section_layer(tokens, gain, query_matrix, keyval_matrix, output_matrix, token_positions)
        produced = layer(forward_tokens)
        unused, back_layer = jax.vjp(layer, saved_tokens)
        token_grads, = back_layer(upstream)
        return (produced, token_grads)
    results, gradients = lax.map(one_section, (section_inputs, saved_inputs, output_grads, norm_gain, query_weight, keyval_weight, output_weight))
    return (jnp.roll(results, 1, axis=0), jnp.roll(gradients, -1, axis=0))
```

```python
import functools

import jax
import jax.numpy as jnp
from jax import lax
from jax.experimental import pallas as pl
from jax.experimental.pallas import tpu as pltpu
from jax.sharding import PartitionSpec as P

HEAD_DIM = 128


norm_eps = 1e-05
rope_base = 500000.0


def from_behind(block, axis, distance):
    devices = range(lax.axis_size(axis))
    route = [((i - distance) % len(devices), i) for i in devices]
    return lax.ppermute(block, axis, route)


def rotate(matrix, positions):
    half_dim = matrix.shape[-1] // 2
    frequency = rope_base ** (-2.0 * jnp.arange(half_dim, dtype=jnp.float32) / matrix.shape[-1])
    angles = positions.astype(jnp.float32)[:, None] * frequency[None, :]
    cos_table = jnp.cos(angles)[:, None, :]
    sin_table = jnp.sin(angles)[:, None, :]
    leading = matrix[..., :half_dim]
    trailing = matrix[..., half_dim:]
    return jnp.concatenate(
        [leading * cos_table - trailing * sin_table, trailing * cos_table + leading * sin_table],
        axis=-1,
    )


def project(tokens, gain, query_matrix, keyval_matrix, positions):
    widened = tokens.astype(jnp.float32)
    inverse = lax.rsqrt(jnp.mean(widened * widened, axis=-1, keepdims=True) + norm_eps)
    normed = (widened * inverse * gain[None, :]).astype(jnp.bfloat16)
    row_count = tokens.shape[0]
    query_full = jnp.dot(normed, query_matrix, preferred_element_type=jnp.float32)
    keyval_full = jnp.dot(normed, keyval_matrix, preferred_element_type=jnp.float32)
    queries = rotate(query_full.reshape(row_count, -1, HEAD_DIM), positions).astype(jnp.bfloat16)
    paired = keyval_full.reshape(row_count, 2, -1, HEAD_DIM)
    key_rows = rotate(paired[:, 0], positions).astype(jnp.bfloat16)
    value_rows = paired[:, 1].astype(jnp.bfloat16)
    return (queries, key_rows, value_rows)


def attend(queries, key_wide, value_wide, query_pos, key_pos, narrow):
    row_count = queries.shape[0]
    kv_count = key_wide.shape[1]
    head_size = queries.shape[2]
    group_size = queries.shape[1] // kv_count
    grouped = jnp.moveaxis(queries.reshape(row_count, kv_count, group_size, head_size), 1, 0)
    key_heads = jnp.moveaxis(key_wide, 1, 0)
    value_heads = jnp.moveaxis(value_wide, 1, 0)
    visible = (key_pos[None, :] <= query_pos[:, None])[None]

    def one_head(block):
        query_block, key_block, value_block = block
        scores = jnp.einsum(
            "rgd,sd->grs", query_block, key_block, preferred_element_type=jnp.float32
        ) * head_size ** (-0.5)
        masked = jnp.where(visible, scores, -1e30)
        row_max = lax.stop_gradient(jnp.max(masked, axis=-1, keepdims=True))
        numerators = jnp.where(visible, jnp.exp(masked - row_max), 0.0)
        totals = jnp.sum(numerators, axis=-1)
        if narrow:
            rounded = numerators.astype(jnp.bfloat16)
        else:
            rounded = lax.optimization_barrier(numerators.astype(jnp.bfloat16)).astype(jnp.float32)
        summed = jnp.einsum("grs,sd->rgd", rounded, value_block, preferred_element_type=jnp.float32)
        return summed / jnp.transpose(totals, (1, 0))[..., None]

    averaged = lax.map(one_head, (grouped, key_heads, value_heads))
    return jnp.moveaxis(averaged, 0, 1).reshape(row_count, -1).astype(jnp.bfloat16)


def finish(tokens, mixed, output_matrix):
    return (
        tokens.astype(jnp.float32)
        + jnp.dot(mixed, output_matrix, preferred_element_type=jnp.float32)
    ).astype(jnp.bfloat16)


def shards(
    section_inputs,
    saved_inputs,
    output_grads,
    token_positions,
    norm_gain,
    query_weight,
    keyval_weight,
    output_weight,
):
    key_positions = lax.all_gather(token_positions, "ctx", axis=0, tiled=True)
    full_query, full_keyval = (
        lax.all_gather(query_weight[0], "ctx", axis=0, tiled=True),
        lax.all_gather(keyval_weight[0], "ctx", axis=0, tiled=True),
    )
    full_output = output_weight[0]
    gain = norm_gain[0]
    forward_tokens = section_inputs[0]
    saved_tokens = saved_inputs[0]
    upstream = output_grads[0]

    def projector(tokens):
        return project(tokens, gain, full_query, full_keyval, token_positions)

    def attention_wide(queries, key_wide, value_wide):
        return attend(queries, key_wide, value_wide, token_positions, key_positions, False)

    def finishing(tokens, mixed):
        return finish(tokens, mixed, full_output)

    forward_queries, forward_keys, forward_values = projector(forward_tokens)
    (backward_queries, backward_keys, backward_values), back_project = jax.vjp(
        projector, saved_tokens
    )
    forward_keyset, forward_valueset = (
        lax.all_gather(forward_keys, "ctx", axis=0, tiled=True),
        lax.all_gather(forward_values, "ctx", axis=0, tiled=True),
    )
    mixed = attend(
        forward_queries, forward_keyset, forward_valueset, token_positions, key_positions, True
    )
    produced = finishing(forward_tokens, mixed)
    sent_on = from_behind(produced[None], "section", 1)
    backward_keyset, backward_valueset = (
        lax.all_gather(backward_keys, "ctx", axis=0, tiled=True),
        lax.all_gather(backward_values, "ctx", axis=0, tiled=True),
    )
    mixed, back_attend = jax.vjp(
        attention_wide,
        backward_queries.astype(jnp.float32),
        backward_keyset.astype(jnp.float32),
        backward_valueset.astype(jnp.float32),
    )
    produced, back_finish = jax.vjp(finishing, saved_tokens, mixed)
    residual_grad, mixed_grad = back_finish(upstream)
    query_grad, key_partial, value_partial = back_attend(mixed_grad)
    key_grads = lax.psum_scatter(
        key_partial.astype(jnp.bfloat16), "ctx", scatter_dimension=0, tiled=True
    )
    value_grads = lax.psum_scatter(
        value_partial.astype(jnp.bfloat16), "ctx", scatter_dimension=0, tiled=True
    )
    (project_grad,) = back_project((query_grad.astype(jnp.bfloat16), key_grads, value_grads))
    sent_back = from_behind((residual_grad + project_grad)[None], "section", -1)
    return (sent_on, sent_back)


MESH = pl.DeviceIdType.MESH
VMEM = pl.BlockSpec(memory_space=pltpu.VMEM)
ANY = pl.BlockSpec(memory_space=pl.ANY)
WIDE = jnp.float32
SLIM = jnp.bfloat16


def remote(src, dst, send, recv, device):
    return pltpu.make_async_remote_copy(
        src_ref=src, dst_ref=dst, send_sem=send, recv_sem=recv, device_id=device, device_id_type=MESH
    )


def sides(n, me, section):
    for t in range(1, n):
        for side, other, fits in ((0, me + t, me + t < n), (1, me - t, me - t >= 0)):
            yield side, t, fits, other


def gather_kernel(
    n, nf, nb, up, wo_hbm, wq, wkv, pos, qkv_f, qkv_b, mg, wh, posg,
    xf, xb, mgl, wo, xsend, xrecv, wsend, wrecv, msend, mrecv, psend, precv, own,
):
    section = lax.axis_index("section")
    me = lax.axis_index("ctx")
    depth, _ = wq.shape
    gq = mg.shape[2]
    wide = wh.shape[2]
    kvw = (wide - gq) // 2
    half = kvw * n

    barrier = pltpu.get_barrier_semaphore()
    for k in range(1, n):
        pl.semaphore_signal(barrier, inc=1, device_id=(section, lax.rem(me + k, n)), device_id_type=MESH)
    pl.semaphore_wait(barrier, n - 1)

    def weight_copies(side, t, target, source):
        parts = (
            (wq, target * gq, gq, 0),
            (wkv, target * kvw, kvw, gq),
            (wkv, half + target * kvw, kvw, gq + kvw),
        )
        return [
            remote(
                ref.at[:, pl.ds(pl.multiple_of(start, 128), size)],
                wh.at[source, :, pl.ds(to, size)],
                wsend.at[side, t, i], wrecv.at[side, t, i], (section, target),
            )
            for i, (ref, start, size, to) in enumerate(parts)
        ]

    def row_copies(side, t, block, target):
        pairs = ((nf, xf), (nb, xb))
        return [
            remote(
                first if t == 1 else every.at[block], every.at[block],
                xsend.at[side, t, i], xrecv.at[side, t, i], (section, target),
            )
            for i, (first, every) in enumerate(pairs)
        ]

    def small_copies(side, t, target):
        return [remote(mgl.at[target], mg.at[me], msend.at[side, t], mrecv.at[side, t], (section, target))]

    def place_copies(side, t, target):
        return [remote(pos, posg.at[me], psend.at[side, t], precv.at[side, t], (section, target))]

    def begin(copies):
        for copy in copies:
            copy.start()

    def next_on(side):
        return (me + 1, me + 1 < n) if side == 0 else (me - 1, me - 1 >= 0)

    def behind(side, t):
        return (me - t, me - t >= 0) if side == 0 else (me + t, me + t < n)

    for side in (0, 1):
        target, fits = next_on(side)
        pl.when(fits)(lambda side=side, target=target: begin(row_copies(side, 1, me, target)))
    for side, t, fits, other in sides(n, me, section):
        pl.when(fits)(lambda side=side, t=t, other=other: begin(place_copies(side, t, other)))
    wo_copy = pltpu.make_async_copy(wo_hbm, wo, own.at[0])
    wo_copy.start()
    mine = [
        pltpu.make_async_copy(
            ref.at[:, pl.ds(pl.multiple_of(start, 128), size)], wh.at[me, :, pl.ds(to, size)], own.at[i + 1]
        )
        for i, (ref, start, size, to) in enumerate(
            ((wq, me * gq, gq, 0), (wkv, me * kvw, kvw, gq), (wkv, half + me * kvw, kvw, gq + kvw))
        )
    ]
    begin(mine)
    xf[me] = nf[...]
    xb[me] = nb[...]
    posg[me] = pos[...]

    def send_weights(t):
        for side, other, fits in ((0, me + t, me + t < n), (1, me - t, me - t >= 0)):
            pl.when(fits)(
                lambda side=side, other=other: begin(weight_copies(side, t, other, me))
            )

    send_weights(1)
    wo_copy.wait()
    for j in range(n):
        mgl[j] = lax.dot_general(
            up[...], wo[pl.ds(j * gq, gq), :], (((1,), (1,)), ((), ())), preferred_element_type=WIDE
        ).astype(SLIM)
    mg[me] = mgl[me]
    for t in range(1, n):
        if t > 1:
            send_weights(t)
        for side in (0, 1):
            block, there = behind(side, t)
            target, fits = next_on(side)

            @pl.when(there)
            def _():
                for copy in row_copies(side, t, block, me):
                    copy.wait_recv()

            if t + 1 < n:
                pl.when(jnp.logical_and(there, fits))(
                    lambda side=side, target=target, block=block: begin(
                        row_copies(side, t + 1, block, target)
                    )
                )
    for side, t, fits, other in sides(n, me, section):
        pl.when(fits)(lambda side=side, t=t, other=other: begin(small_copies(side, t, other)))

    tile = 256 if wide % 256 == 0 else 128

    def add_from(j, first):
        columns = pl.ds(pl.multiple_of(j * depth, 128), depth)

        @pl.loop(0, wide // tile)
        def _(c):
            at = pl.ds(pl.multiple_of(c * tile, 128), tile)
            weights = wh[j, :, at]
            for every, total in ((xf, qkv_f), (xb, qkv_b)):
                rows = every[:, :, columns].reshape(-1, depth)
                term = jnp.dot(rows, weights, preferred_element_type=WIDE)
                total[:, at] = term if first else total[:, at] + term

    for copy in mine:
        copy.wait()
    add_from(me, True)
    for t in range(1, n):
        for side in (0, 1):
            block, there = behind(side, t)

            @pl.when(there)
            def _():
                for copy in weight_copies(side, t, me, block):
                    copy.wait_recv()
                add_from(block, False)

    for t in range(1, n):
        for side in (0, 1):
            block, there = behind(side, t)

            @pl.when(there)
            def _():
                for copy in small_copies(side, t, me) + place_copies(side, t, me):
                    copy.wait_recv()

    for side, t, fits, other in sides(n, me, section):

        @pl.when(fits)
        def _():
            for copy in (
                weight_copies(side, t, other, me) + small_copies(side, t, other) + place_copies(side, t, other)
            ):
                copy.wait_send()

    for t in range(1, n):
        for side in (0, 1):
            block, there = behind(side, t - 1)
            target, fits = next_on(side)

            @pl.when(jnp.logical_and(there, fits))
            def _():
                for copy in row_copies(side, t, block, target):
                    copy.wait_send()


def attend_kernel(qkv_f, qkv_b, mg, cos, sin, qpos, kpos, mixed, dqkv):
    gq = mg.shape[1]
    kvw = (qkv_f.shape[1] - gq) // 2
    group = gq // kvw
    scale = HEAD_DIM ** (-0.5)
    visible = kpos[...] <= qpos[...]

    def turn(block, sign):
        return block * cos[...] + sign * (pltpu.roll(block, HEAD_DIM // 2, 1) * sin[...])

    def dot(a, b, dims):
        return lax.dot_general(a, b, (dims, ((), ())), preferred_element_type=WIDE)

    def weigh(queries, keys):
        scores = dot(queries, keys, ((1,), (1,))) * scale
        masked = jnp.where(visible, scores, -1e30)
        row_max = jnp.max(masked, axis=-1, keepdims=True)
        numerators = jnp.where(visible, jnp.exp(masked - row_max), 0.0)
        return numerators, jnp.sum(numerators, axis=-1, keepdims=True)

    for kv in range(kvw // HEAD_DIM):
        key_at = pl.ds(gq + kv * HEAD_DIM, HEAD_DIM)
        value_at = pl.ds(gq + kvw + kv * HEAD_DIM, HEAD_DIM)
        keys_f, values_f = turn(qkv_f[:, key_at], 1.0).astype(SLIM), qkv_f[:, value_at].astype(SLIM)
        keys_b, values_b = turn(qkv_b[:, key_at], 1.0).astype(SLIM), qkv_b[:, value_at].astype(SLIM)

        def head(h, grads):
            at = pl.ds(pl.multiple_of((kv * group + h) * HEAD_DIM, HEAD_DIM), HEAD_DIM)
            queries = turn(qkv_f[:, at], 1.0).astype(SLIM)
            numerators, totals = weigh(queries, keys_f)
            mixed[:, at] = (dot(numerators.astype(SLIM), values_f, ((1,), (0,))) / totals).astype(SLIM)

            queries = turn(qkv_b[:, at], 1.0).astype(SLIM)
            numerators, totals = weigh(queries, keys_b)
            rounded = numerators.astype(SLIM)
            summed = dot(rounded, values_b, ((1,), (0,)))
            grad = mg[:, at].astype(WIDE)
            summed_grad = grad / totals
            totals_grad = -jnp.sum(summed_grad * (summed / totals), axis=-1, keepdims=True)
            narrow_grad = summed_grad.astype(SLIM)
            numer_grad = dot(narrow_grad, values_b, ((1,), (1,))) + totals_grad
            score_grad = (numerators * numer_grad * scale).astype(SLIM)
            query_grad = dot(score_grad, keys_b, ((1,), (0,))).astype(SLIM)
            dqkv[:, at] = turn(query_grad.astype(WIDE), -1.0).astype(SLIM)
            key_grad, value_grad = grads
            return (
                key_grad + dot(score_grad, queries, ((0,), (0,))),
                value_grad + dot(rounded, narrow_grad, ((0,), (0,))),
            )

        nothing = jnp.zeros(keys_b.shape, WIDE)
        key_grad, value_grad = lax.fori_loop(0, group, head, (nothing, nothing))
        dqkv[:, key_at] = turn(key_grad.astype(SLIM).astype(WIDE), -1.0).astype(SLIM)
        dqkv[:, value_at] = value_grad.astype(SLIM)


def finish_kernel(
    n, sections, mixed, dqkv, wh, wo_hbm, tokens, saved, upstream, gain, ahead, back,
    mixed_in, part, part_in, wo, produced, grads, asend, arecv, bsend, brecv, csend, crecv, own,
):
    section = lax.axis_index("section")
    me = lax.axis_index("ctx")
    gq = mixed.shape[2]
    depth = wh.shape[1]
    following, preceding = lax.rem(section + 1, sections), lax.rem(section + sections - 1, sections)

    barrier = pltpu.get_barrier_semaphore()
    for k in range(1, n):
        pl.semaphore_signal(barrier, inc=1, device_id=(section, lax.rem(me + k, n)), device_id_type=MESH)
    for other in (following, preceding):
        pl.semaphore_signal(barrier, inc=1, device_id=(other, me), device_id_type=MESH)
    pl.semaphore_wait(barrier, n + 1)

    wo_copy = pltpu.make_async_copy(wo_hbm, wo, own)
    wo_copy.start()

    def mixed_copy(k, target):
        return remote(mixed.at[target], mixed_in.at[k], asend.at[k], arecv.at[k], (section, target))

    def part_copy(k, target):
        return remote(part.at[k], part_in.at[k], bsend.at[k], brecv.at[k], (section, target))

    order = [n // 2] + [k for k in range(1, n) if k != n // 2]
    for k in order:
        mixed_copy(k, lax.rem(me + k, n)).start()

    def partial_grad(target, k):
        rows = dqkv[target]
        for j in range(n):
            part[k, :, pl.ds(j * depth, depth)] = lax.dot_general(
                rows, wh[j], (((1,), (1,)), ((), ())), preferred_element_type=WIDE
            ).astype(SLIM)

    for k in order:
        target = lax.rem(me + k, n)
        partial_grad(target, k)
        part_copy(k, target).start()
    partial_grad(me, 0)
    wo_copy.wait()

    def from_source(k):
        return lax.rem(me + n - k, n)

    total = tokens[...].astype(WIDE)
    total += jnp.dot(
        mixed[me], wo[pl.ds(pl.multiple_of(me * gq, 128), gq), :], preferred_element_type=WIDE
    )
    for k in range(1, n):
        mixed_copy(k, me).wait_recv()
        rows = pl.ds(pl.multiple_of(from_source(k) * gq, 128), gq)
        total += jnp.dot(mixed_in[k], wo[rows, :], preferred_element_type=WIDE)
    produced[...] = total.astype(SLIM)

    ahead_copy = remote(produced, ahead, csend.at[0], crecv.at[0], (following, me))
    ahead_copy.start()

    widened = saved[...].astype(WIDE)
    inverse = lax.rsqrt(jnp.mean(widened * widened, axis=-1, keepdims=True) + norm_eps)
    normed_grad = part[0].astype(WIDE)
    for k in range(1, n):
        part_copy(k, me).wait_recv()
        normed_grad += part_in[k].astype(WIDE)
    scaled = normed_grad.astype(SLIM).astype(WIDE) * gain[...]
    inner = jnp.mean(scaled * widened, axis=-1, keepdims=True)
    project_grad = inverse * scaled - widened * (inverse * inverse * inverse * inner)
    grads[...] = upstream[...] + project_grad.astype(SLIM)

    back_copy = remote(grads, back, csend.at[1], crecv.at[1], (preceding, me))
    back_copy.start()
    for k in range(1, n):
        mixed_copy(k, lax.rem(me + k, n)).wait_send()
        part_copy(k, lax.rem(me + k, n)).wait_send()
    ahead_copy.wait()
    back_copy.wait()


def by_heads(n, sections):
    def step(
        section_inputs, saved_inputs, output_grads, token_positions, norm_gain,
        query_weight, keyval_weight, output_weight,
    ):
        _, rows, width = section_inputs.shape
        _, depth, query_width = query_weight.shape
        gq = query_width // n
        wide = gq + keyval_weight.shape[2] // n
        limit = 60 * 2**20

        def norm(tokens):
            widened = tokens.astype(WIDE)
            inverse = lax.rsqrt(jnp.mean(widened * widened, axis=-1, keepdims=True) + norm_eps)
            return (widened * inverse * norm_gain).astype(SLIM)

        def shaped(shape, kind=SLIM):
            return jax.ShapeDtypeStruct(shape, kind)

        dma = pltpu.SemaphoreType.DMA
        qkv_f, qkv_b, mixed_grad, head_weights, places = pl.pallas_call(
            functools.partial(gather_kernel, n),
            out_shape=(
                shaped((n * rows, wide), WIDE), shaped((n * rows, wide), WIDE), shaped((n, rows, gq)),
                shaped((n, depth, wide)), shaped((n, 1, rows), jnp.int32),
            ),
            in_specs=[VMEM, VMEM, VMEM, ANY, ANY, ANY, VMEM],
            out_specs=(VMEM,) * 5,
            scratch_shapes=[
                pltpu.VMEM((n, rows, width), SLIM), pltpu.VMEM((n, rows, width), SLIM),
                pltpu.VMEM((n, rows, gq), SLIM), pltpu.VMEM((query_width, width), SLIM),
                dma((2, n, 2)), dma((2, n, 2)), dma((2, n, 3)), dma((2, n, 3)),
                dma((2, n)), dma((2, n)), dma((2, n)), dma((2, n)), dma((4,)),
            ],
            compiler_params=pltpu.CompilerParams(
                collective_id=0, has_side_effects=True, vmem_limit_bytes=limit
            ),
            name="gather",
        )(
            norm(section_inputs[0]), norm(saved_inputs[0]), output_grads[0], output_weight[0],
            query_weight[0], keyval_weight[0], token_positions[None],
        )

        positions = places.reshape(-1)
        half_dim = HEAD_DIM // 2
        frequency = rope_base ** (-2.0 * jnp.arange(half_dim, dtype=WIDE) / HEAD_DIM)
        angles = positions.astype(WIDE)[:, None] * frequency[None, :]
        cos_table, sin_table = jnp.cos(angles), jnp.sin(angles)
        cos_table = jnp.concatenate([cos_table, cos_table], axis=-1)
        sin_table = jnp.concatenate([-sin_table, sin_table], axis=-1)
        mixed, qkv_grad = pl.pallas_call(
            attend_kernel,
            out_shape=(shaped((n * rows, gq)), shaped((n * rows, wide))),
            in_specs=[VMEM] * 7,
            out_specs=(VMEM,) * 2,
            compiler_params=pltpu.CompilerParams(vmem_limit_bytes=limit),
            name="attend",
        )(
            qkv_f, qkv_b, mixed_grad.reshape(n * rows, gq), cos_table, sin_table,
            positions[:, None], positions[None, :],
        )

        ahead, back = pl.pallas_call(
            functools.partial(finish_kernel, n, sections),
            out_shape=(shaped((rows, width)), shaped((rows, width))),
            in_specs=[VMEM, VMEM, VMEM, ANY, VMEM, VMEM, VMEM, VMEM],
            out_specs=(VMEM,) * 2,
            scratch_shapes=[
                pltpu.VMEM((n, rows, gq), SLIM), pltpu.VMEM((n, rows, width), SLIM),
                pltpu.VMEM((n, rows, width), SLIM), pltpu.VMEM((query_width, width), SLIM),
                pltpu.VMEM((rows, width), SLIM), pltpu.VMEM((rows, width), SLIM),
                dma((n,)), dma((n,)), dma((n,)), dma((n,)), dma((2,)), dma((2,)), dma,
            ],
            compiler_params=pltpu.CompilerParams(
                collective_id=1, has_side_effects=True, vmem_limit_bytes=limit
            ),
            name="finish",
        )(
            mixed.reshape(n, rows, gq), qkv_grad.reshape(n, rows, wide), head_weights, output_weight[0],
            section_inputs[0], saved_inputs[0], output_grads[0], norm_gain,
        )
        return (ahead[None], back[None])

    return step


def solution(mesh):
    placed = (
        P("section", "ctx", None),
        P("section", "ctx", None),
        P("section", "ctx", None),
        P("ctx"),
        P("section", None),
        P("section", "ctx", None),
        P("section", "ctx", None),
        P("section", None, None),
    )
    n, sections = mesh.shape["ctx"], mesh.shape["section"]

    def chosen(*blocks):
        kv_heads = blocks[6].shape[2] // (2 * HEAD_DIM)
        if n > 1 and sections > 2 and kv_heads % n == 0:
            return by_heads(n, sections)(*blocks)
        return shards(*blocks)

    return jax.shard_map(
        chosen,
        mesh=mesh,
        in_specs=placed,
        out_specs=(P("section", "ctx", None), P("section", "ctx", None)),
        check_vma=False,
    )
```

```python
import functools

import jax
import jax.numpy as jnp
from jax import lax
from jax.experimental import pallas as pl
from jax.experimental.pallas import tpu as pltpu
from jax.sharding import PartitionSpec as P

HEAD_DIM = 128


norm_eps = 1e-05
rope_base = 500000.0


def from_behind(block, axis, distance):
    devices = range(lax.axis_size(axis))
    route = [((i - distance) % len(devices), i) for i in devices]
    return lax.ppermute(block, axis, route)


def rotate(matrix, positions):
    half_dim = matrix.shape[-1] // 2
    frequency = rope_base ** (-2.0 * jnp.arange(half_dim, dtype=jnp.float32) / matrix.shape[-1])
    angles = positions.astype(jnp.float32)[:, None] * frequency[None, :]
    cos_table = jnp.cos(angles)[:, None, :]
    sin_table = jnp.sin(angles)[:, None, :]
    leading = matrix[..., :half_dim]
    trailing = matrix[..., half_dim:]
    return jnp.concatenate(
        [leading * cos_table - trailing * sin_table, trailing * cos_table + leading * sin_table],
        axis=-1,
    )


def project(tokens, gain, query_matrix, keyval_matrix, positions):
    widened = tokens.astype(jnp.float32)
    inverse = lax.rsqrt(jnp.mean(widened * widened, axis=-1, keepdims=True) + norm_eps)
    normed = (widened * inverse * gain[None, :]).astype(jnp.bfloat16)
    row_count = tokens.shape[0]
    query_full = jnp.dot(normed, query_matrix, preferred_element_type=jnp.float32)
    keyval_full = jnp.dot(normed, keyval_matrix, preferred_element_type=jnp.float32)
    queries = rotate(query_full.reshape(row_count, -1, HEAD_DIM), positions).astype(jnp.bfloat16)
    paired = keyval_full.reshape(row_count, 2, -1, HEAD_DIM)
    key_rows = rotate(paired[:, 0], positions).astype(jnp.bfloat16)
    value_rows = paired[:, 1].astype(jnp.bfloat16)
    return (queries, key_rows, value_rows)


def attend(queries, key_wide, value_wide, query_pos, key_pos, narrow):
    row_count = queries.shape[0]
    kv_count = key_wide.shape[1]
    head_size = queries.shape[2]
    group_size = queries.shape[1] // kv_count
    grouped = jnp.moveaxis(queries.reshape(row_count, kv_count, group_size, head_size), 1, 0)
    key_heads = jnp.moveaxis(key_wide, 1, 0)
    value_heads = jnp.moveaxis(value_wide, 1, 0)
    visible = (key_pos[None, :] <= query_pos[:, None])[None]

    def one_head(block):
        query_block, key_block, value_block = block
        scores = jnp.einsum(
            "rgd,sd->grs", query_block, key_block, preferred_element_type=jnp.float32
        ) * head_size ** (-0.5)
        masked = jnp.where(visible, scores, -1e30)
        row_max = lax.stop_gradient(jnp.max(masked, axis=-1, keepdims=True))
        numerators = jnp.where(visible, jnp.exp(masked - row_max), 0.0)
        totals = jnp.sum(numerators, axis=-1)
        if narrow:
            rounded = numerators.astype(jnp.bfloat16)
        else:
            rounded = lax.optimization_barrier(numerators.astype(jnp.bfloat16)).astype(jnp.float32)
        summed = jnp.einsum("grs,sd->rgd", rounded, value_block, preferred_element_type=jnp.float32)
        return summed / jnp.transpose(totals, (1, 0))[..., None]

    averaged = lax.map(one_head, (grouped, key_heads, value_heads))
    return jnp.moveaxis(averaged, 0, 1).reshape(row_count, -1).astype(jnp.bfloat16)


def finish(tokens, mixed, output_matrix):
    return (
        tokens.astype(jnp.float32)
        + jnp.dot(mixed, output_matrix, preferred_element_type=jnp.float32)
    ).astype(jnp.bfloat16)


def shards(
    section_inputs,
    saved_inputs,
    output_grads,
    token_positions,
    norm_gain,
    query_weight,
    keyval_weight,
    output_weight,
):
    key_positions = lax.all_gather(token_positions, "ctx", axis=0, tiled=True)
    full_query, full_keyval = (
        lax.all_gather(query_weight[0], "ctx", axis=0, tiled=True),
        lax.all_gather(keyval_weight[0], "ctx", axis=0, tiled=True),
    )
    full_output = output_weight[0]
    gain = norm_gain[0]
    forward_tokens = section_inputs[0]
    saved_tokens = saved_inputs[0]
    upstream = output_grads[0]

    def projector(tokens):
        return project(tokens, gain, full_query, full_keyval, token_positions)

    def attention_wide(queries, key_wide, value_wide):
        return attend(queries, key_wide, value_wide, token_positions, key_positions, False)

    def finishing(tokens, mixed):
        return finish(tokens, mixed, full_output)

    forward_queries, forward_keys, forward_values = projector(forward_tokens)
    (backward_queries, backward_keys, backward_values), back_project = jax.vjp(
        projector, saved_tokens
    )
    forward_keyset, forward_valueset = (
        lax.all_gather(forward_keys, "ctx", axis=0, tiled=True),
        lax.all_gather(forward_values, "ctx", axis=0, tiled=True),
    )
    mixed = attend(
        forward_queries, forward_keyset, forward_valueset, token_positions, key_positions, True
    )
    produced = finishing(forward_tokens, mixed)
    sent_on = from_behind(produced[None], "section", 1)
    backward_keyset, backward_valueset = (
        lax.all_gather(backward_keys, "ctx", axis=0, tiled=True),
        lax.all_gather(backward_values, "ctx", axis=0, tiled=True),
    )
    mixed, back_attend = jax.vjp(
        attention_wide,
        backward_queries.astype(jnp.float32),
        backward_keyset.astype(jnp.float32),
        backward_valueset.astype(jnp.float32),
    )
    produced, back_finish = jax.vjp(finishing, saved_tokens, mixed)
    residual_grad, mixed_grad = back_finish(upstream)
    query_grad, key_partial, value_partial = back_attend(mixed_grad)
    key_grads = lax.psum_scatter(
        key_partial.astype(jnp.bfloat16), "ctx", scatter_dimension=0, tiled=True
    )
    value_grads = lax.psum_scatter(
        value_partial.astype(jnp.bfloat16), "ctx", scatter_dimension=0, tiled=True
    )
    (project_grad,) = back_project((query_grad.astype(jnp.bfloat16), key_grads, value_grads))
    sent_back = from_behind((residual_grad + project_grad)[None], "section", -1)
    return (sent_on, sent_back)


MESH = pl.DeviceIdType.MESH
VMEM = pl.BlockSpec(memory_space=pltpu.VMEM)
ANY = pl.BlockSpec(memory_space=pl.ANY)
WIDE = jnp.float32
SLIM = jnp.bfloat16


def remote(src, dst, send, recv, device):
    return pltpu.make_async_remote_copy(
        src_ref=src, dst_ref=dst, send_sem=send, recv_sem=recv, device_id=device, device_id_type=MESH
    )


def layer_kernel(
    n, sections, nf, nb, up, wo_hbm, wq, wkv, pos, waves, tokens, saved, gain, ahead, back,
    xf, xb, mgl, mg, wo, wh, posg, qcol, cos, sin, qkv_f, qkv_b, mixed, dqkv, mixed_in, part, inbox,
    produced, grads, fsend, frecv, gsend, grecv, wsend, wrecv, msend, mrecv, psend, precv,
    asend, arecv, bsend, brecv, csend, crecv, own,
):
    section = lax.axis_index("section")
    me = lax.axis_index("ctx")
    depth, _ = wq.shape
    rows, gq = mg.shape[1:]
    wide = wh.shape[2]
    kvw = (wide - gq) // 2
    half = kvw * n
    group = gq // kvw
    scale = HEAD_DIM ** (-0.5)
    following, preceding = lax.rem(section + 1, sections), lax.rem(section + sections - 1, sections)

    barrier = pltpu.get_barrier_semaphore()
    for k in range(1, n):
        pl.semaphore_signal(barrier, inc=1, device_id=(section, lax.rem(me + k, n)), device_id_type=MESH)
    for other in (following, preceding):
        pl.semaphore_signal(barrier, inc=1, device_id=(other, me), device_id_type=MESH)
    pl.semaphore_wait(barrier, n + 1)

    def peer(side, t):
        return (me + t, me + t < n) if side == 0 else (me - t, me - t >= 0)

    def behind(side, t):
        return peer(1 - side, t)

    def begin(copies):
        for copy in copies:
            copy.start()

    def arrive(copies):
        for copy in copies:
            copy.wait_recv()

    def leave(copies):
        for copy in copies:
            copy.wait_send()

    def weight_copies(side, t, target, source):
        parts = (
            (wq, target * gq, gq, 0),
            (wkv, target * kvw, kvw, gq),
            (wkv, half + target * kvw, kvw, gq + kvw),
        )
        return [
            remote(
                ref.at[:, pl.ds(pl.multiple_of(start, 128), size)],
                wh.at[source, :, pl.ds(to, size)],
                wsend.at[side, t, i], wrecv.at[side, t, i], (section, target),
            )
            for i, (ref, start, size, to) in enumerate(parts)
        ]

    relays = ((nf, xf, fsend, frecv), (nb, xb, gsend, grecv))

    def row_copies(batch, side, t, block, target):
        first, every, send, recv = relays[batch]
        return [
            remote(
                first if t == 1 else every.at[block], every.at[block],
                send.at[side, t], recv.at[side, t], (section, target),
            )
        ]

    def small_copies(side, t, target):
        return [remote(mgl.at[target], mg.at[me], msend.at[side, t], mrecv.at[side, t], (section, target))]

    def place_copies(side, t, target):
        return [remote(pos, posg.at[me], psend.at[side, t], precv.at[side, t], (section, target))]

    def mixed_copies(side, t, target):
        return [
            remote(mixed.at[target], mixed_in.at[me], asend.at[side, t], arecv.at[side, t], (section, target))
        ]

    def hop(batch, side, t):
        block, there = behind(side, t)
        target, fits = peer(side, 1)
        pl.when(there)(lambda: arrive(row_copies(batch, side, t, block, me)))
        if t + 1 < n:
            pl.when(jnp.logical_and(there, fits))(
                lambda: begin(row_copies(batch, side, t + 1, block, target))
            )

    def send_own(batch):
        for side in (0, 1):
            target, fits = peer(side, 1)
            pl.when(fits)(lambda: begin(row_copies(batch, side, 1, me, target)))

    def to_all(copies, action):
        for t in range(n - 1, 0, -1):
            for side in (0, 1):
                target, fits = peer(side, t)
                pl.when(fits)(lambda: action(copies(side, t, target)))

    def from_all(copies):
        for t in range(1, n):
            for side in (0, 1):
                _, there = behind(side, t)
                pl.when(there)(lambda: arrive(copies(side, t, me)))

    send_own(0)
    to_all(place_copies, begin)
    wo_copy = pltpu.make_async_copy(wo_hbm, wo, own.at[0])
    wo_copy.start()
    mine = [
        pltpu.make_async_copy(
            ref.at[:, pl.ds(pl.multiple_of(start, 128), size)], wh.at[me, :, pl.ds(to, size)], own.at[i + 1]
        )
        for i, (ref, start, size, to) in enumerate(
            ((wq, me * gq, gq, 0), (wkv, me * kvw, kvw, gq), (wkv, half + me * kvw, kvw, gq + kvw))
        )
    ]
    begin(mine)
    posg[me] = pos[...]
    xf[me] = nf[...]
    xb[me] = nb[...]

    def send_weights(side):
        for t in range(n - 1, 0, -1):
            target, fits = peer(side, t)
            pl.when(fits)(lambda: begin(weight_copies(side, t, target, me)))

    for t in range(1, n):
        pl.when(me == t - 1)(lambda: send_weights(0))
        pl.when(n - me == t)(lambda: send_weights(1))
        for side in (0, 1):
            hop(0, side, t)

    wo_copy.wait()
    for j in range(n):
        mgl[j] = lax.dot_general(
            up[...], wo[pl.ds(j * gq, gq), :], (((1,), (1,)), ((), ())), preferred_element_type=WIDE
        ).astype(SLIM)
    mg[me] = mgl[me]
    send_own(1)
    to_all(small_copies, begin)

    from_all(place_copies)
    for j in range(n):
        column = jnp.transpose(jnp.broadcast_to(posg[j].astype(WIDE), (HEAD_DIM, rows)))
        angles = column * waves[0:1, :]
        qcol[j] = column
        cos[pl.ds(j * rows, rows), :] = jnp.cos(angles)
        sin[pl.ds(j * rows, rows), :] = jnp.sin(angles) * waves[1:2, :]

    tile = 256 if wide % 256 == 0 else 128

    def add_from(j, first):
        columns = pl.ds(pl.multiple_of(j * depth, 128), depth)

        @pl.loop(0, wide // tile)
        def _(c):
            at = pl.ds(pl.multiple_of(c * tile, 128), tile)
            term = jnp.dot(
                xf[:, :, columns].reshape(-1, depth), wh[j, :, at], preferred_element_type=WIDE
            )
            qkv_f[:, at] = term if first else qkv_f[:, at] + term

    for copy in mine:
        copy.wait()
    add_from(me, True)
    for t in range(1, n):
        for side in (0, 1):
            block, there = behind(side, t)

            @pl.when(there)
            def _():
                arrive(weight_copies(side, t, me, block))
                add_from(block, False)

    column = qcol[...].reshape(n * rows, HEAD_DIM)
    visible = jnp.transpose(column)[0:1, :] <= column[:, 0:1]

    def turn(block, sign):
        return block * cos[...] + sign * (pltpu.roll(block, HEAD_DIM // 2, 1) * sin[...])

    def dot(a, b, dims):
        return lax.dot_general(a, b, (dims, ((), ())), preferred_element_type=WIDE)

    def weigh(queries, keys):
        scores = dot(queries, keys, ((1,), (1,))) * scale
        masked = jnp.where(visible, scores, -1e30)
        row_max = jnp.max(masked, axis=-1, keepdims=True)
        numerators = jnp.where(visible, jnp.exp(masked - row_max), 0.0)
        return numerators, jnp.sum(numerators, axis=-1, keepdims=True)

    def head_at(kv, h):
        return pl.ds(pl.multiple_of((kv * group + h) * HEAD_DIM, HEAD_DIM), HEAD_DIM)

    def keys_and_values(qkv, kv):
        keys = turn(qkv[:, pl.ds(gq + kv * HEAD_DIM, HEAD_DIM)], 1.0).astype(SLIM)
        return keys, qkv[:, pl.ds(gq + kvw + kv * HEAD_DIM, HEAD_DIM)].astype(SLIM)

    for side in (0, 1):
        hop(1, side, 1)
    for kv in range(kvw // HEAD_DIM):
        keys, values = keys_and_values(qkv_f, kv)

        @pl.loop(0, group)
        def _(h):
            at = head_at(kv, h)
            numerators, totals = weigh(turn(qkv_f[:, at], 1.0).astype(SLIM), keys)
            result = dot(numerators.astype(SLIM), values, ((1,), (0,))) / totals
            mixed[:, :, at] = result.astype(SLIM).reshape(n, rows, HEAD_DIM)

    to_all(mixed_copies, begin)

    def rows_of(block):
        @pl.loop(0, wide // tile)
        def _(c):
            at = pl.ds(pl.multiple_of(c * tile, 128), tile)
            total = jnp.zeros((rows, tile), WIDE)
            for j in range(n):
                total += jnp.dot(
                    xb[block, :, pl.ds(j * depth, depth)], wh[j, :, at], preferred_element_type=WIDE
                )
            qkv_b[pl.ds(pl.multiple_of(block * rows, 8), rows), at] = total

    rows_of(me)
    for t in range(1, n):
        for side in (0, 1):
            if t > 1:
                hop(1, side, t)
            block, there = behind(side, t)
            pl.when(there)(lambda: rows_of(block))

    from_all(small_copies)
    for kv in range(kvw // HEAD_DIM):
        keys, values = keys_and_values(qkv_b, kv)

        def head(h, sums):
            at = head_at(kv, h)
            queries = turn(qkv_b[:, at], 1.0).astype(SLIM)
            numerators, totals = weigh(queries, keys)
            rounded = numerators.astype(SLIM)
            summed = dot(rounded, values, ((1,), (0,)))
            summed_grad = mg[:, :, at].reshape(n * rows, HEAD_DIM).astype(WIDE) / totals
            totals_grad = -jnp.sum(summed_grad * (summed / totals), axis=-1, keepdims=True)
            narrow_grad = summed_grad.astype(SLIM)
            numer_grad = dot(narrow_grad, values, ((1,), (1,))) + totals_grad
            score_grad = (numerators * numer_grad * scale).astype(SLIM)
            query_grad = dot(score_grad, keys, ((1,), (0,))).astype(SLIM)
            dqkv[:, at] = turn(query_grad.astype(WIDE), -1.0).astype(SLIM)
            key_grad, value_grad = sums
            return (
                key_grad + dot(score_grad, queries, ((0,), (0,))),
                value_grad + dot(rounded, narrow_grad, ((0,), (0,))),
            )

        nothing = jnp.zeros(keys.shape, WIDE)
        key_grad, value_grad = lax.fori_loop(0, group, head, (nothing, nothing))
        dqkv[:, pl.ds(gq + kv * HEAD_DIM, HEAD_DIM)] = turn(
            key_grad.astype(SLIM).astype(WIDE), -1.0
        ).astype(SLIM)
        dqkv[:, pl.ds(gq + kvw + kv * HEAD_DIM, HEAD_DIM)] = value_grad.astype(SLIM)

    def sum_copy(side, r, block, target):
        return remote(
            part.at[block], inbox.at[side, r - 1], bsend.at[side, r], brecv.at[side, r - 1], (section, target)
        )

    def partial_grad(block, sides_in, r):
        mine_rows = dqkv[pl.ds(pl.multiple_of(block * rows, 16), rows), :]
        for j in range(n):
            part[block, :, pl.ds(j * depth, depth)] = lax.dot_general(
                mine_rows, wh[j], (((1,), (1,)), ((), ())), preferred_element_type=WIDE
            ).astype(SLIM)
        for side in sides_in:
            _, there = behind(side, 1)

            @pl.when(there)
            def _():
                sum_copy(side, r + 1, block, me).wait_recv()
                part[block] = (part[block].astype(WIDE) + inbox[side, r].astype(WIDE)).astype(SLIM)

    def sum_step(r):
        for side in (0, 1):
            block, there = peer(side, r)
            target, _ = peer(side, 1)

            @pl.when(there)
            def _():
                partial_grad(block, (side,), r)
                sum_copy(side, r, block, target).start()

    sum_step(n - 1)
    total = tokens[...].astype(WIDE)
    total += jnp.dot(
        mixed[me], wo[pl.ds(pl.multiple_of(me * gq, 128), gq), :], preferred_element_type=WIDE
    )
    from_all(mixed_copies)
    for k in range(1, n):
        source = lax.rem(me + k, n)
        at = pl.ds(pl.multiple_of(source * gq, 128), gq)
        total += jnp.dot(mixed_in[source], wo[at, :], preferred_element_type=WIDE)
    produced[...] = total.astype(SLIM)
    ahead_copy = remote(produced, ahead, csend.at[0], crecv.at[0], (following, me))
    ahead_copy.start()
    for r in range(n - 2, 0, -1):
        sum_step(r)
    partial_grad(me, (0, 1), 0)

    widened = saved[...].astype(WIDE)
    inverse = lax.rsqrt(jnp.mean(widened * widened, axis=-1, keepdims=True) + norm_eps)
    scaled = part[me].astype(WIDE) * gain[...]
    inner = jnp.mean(scaled * widened, axis=-1, keepdims=True)
    project_grad = inverse * scaled - widened * (inverse * inverse * inverse * inner)
    grads[...] = up[...] + project_grad.astype(SLIM)
    back_copy = remote(grads, back, csend.at[1], crecv.at[1], (preceding, me))
    back_copy.start()

    to_all(lambda side, t, target: weight_copies(side, t, target, me), leave)
    for copies in (small_copies, place_copies, mixed_copies):
        to_all(copies, leave)
    for t in range(1, n):
        for side in (0, 1):
            block, there = behind(side, t - 1)
            target, fits = peer(side, 1)

            @pl.when(jnp.logical_and(there, fits))
            def _():
                for batch in (0, 1):
                    leave(row_copies(batch, side, t, block, target))

            block, there = peer(side, t)
            pl.when(there)(lambda: leave([sum_copy(side, t, block, target)]))
    ahead_copy.wait()
    back_copy.wait()


def by_heads(n, sections):
    def step(
        section_inputs, saved_inputs, output_grads, token_positions, norm_gain,
        query_weight, keyval_weight, output_weight,
    ):
        _, rows, width = section_inputs.shape
        _, depth, query_width = query_weight.shape
        gq = query_width // n
        wide = gq + keyval_weight.shape[2] // n

        def norm(tokens):
            widened = tokens.astype(WIDE)
            inverse = lax.rsqrt(jnp.mean(widened * widened, axis=-1, keepdims=True) + norm_eps)
            return (widened * inverse * norm_gain).astype(SLIM)

        half_dim = HEAD_DIM // 2
        frequency = rope_base ** (-2.0 * jnp.arange(half_dim, dtype=WIDE) / HEAD_DIM)
        signs = jnp.ones(half_dim, WIDE)
        waves = jnp.stack(
            [jnp.concatenate([frequency, frequency]), jnp.concatenate([-signs, signs])]
        )

        def shaped(shape, kind=SLIM):
            return jax.ShapeDtypeStruct(shape, kind)

        def held(*shape, kind=SLIM):
            return pltpu.VMEM(shape, kind)

        dma = pltpu.SemaphoreType.DMA
        ahead, back = pl.pallas_call(
            functools.partial(layer_kernel, n, sections),
            out_shape=(shaped((rows, width)), shaped((rows, width))),
            in_specs=[VMEM, VMEM, VMEM, ANY, ANY, ANY, VMEM, VMEM, VMEM, VMEM, VMEM],
            out_specs=(VMEM,) * 2,
            scratch_shapes=[
                held(n, rows, width), held(n, rows, width),
                held(n, rows, gq), held(n, rows, gq), held(query_width, width), held(n, depth, wide),
                held(n, 1, rows, kind=jnp.int32), held(n, rows, HEAD_DIM, kind=WIDE),
                held(n * rows, HEAD_DIM, kind=WIDE), held(n * rows, HEAD_DIM, kind=WIDE),
                held(n * rows, wide, kind=WIDE), held(n * rows, wide, kind=WIDE),
                held(n, rows, gq), held(n * rows, wide), held(n, rows, gq),
                held(n, rows, width), held(2, n, rows, width),
                held(rows, width), held(rows, width),
                *[dma((2, n))] * 4, *[dma((2, n, 3))] * 2, *[dma((2, n))] * 8, *[dma((2,))] * 2, dma((4,)),
            ],
            compiler_params=pltpu.CompilerParams(
                collective_id=0, has_side_effects=True, vmem_limit_bytes=60 * 2**20
            ),
            name="layer",
        )(
            norm(section_inputs[0]), norm(saved_inputs[0]), output_grads[0], output_weight[0],
            query_weight[0], keyval_weight[0], token_positions[None], waves,
            section_inputs[0], saved_inputs[0], norm_gain,
        )
        return (ahead[None], back[None])

    return step


def solution(mesh):
    placed = (
        P("section", "ctx", None),
        P("section", "ctx", None),
        P("section", "ctx", None),
        P("ctx"),
        P("section", None),
        P("section", "ctx", None),
        P("section", "ctx", None),
        P("section", None, None),
    )
    n, sections = mesh.shape["ctx"], mesh.shape["section"]

    def chosen(*blocks):
        kv_heads = blocks[6].shape[2] // (2 * HEAD_DIM)
        if n > 1 and sections > 2 and kv_heads % n == 0:
            return by_heads(n, sections)(*blocks)
        return shards(*blocks)

    return jax.shard_map(
        chosen,
        mesh=mesh,
        in_specs=placed,
        out_specs=(P("section", "ctx", None), P("section", "ctx", None)),
        check_vma=False,
    )
```

```python
import functools

import jax
import jax.numpy as jnp
import numpy as np
from jax import lax
from jax.experimental import pallas as pl
from jax.experimental.pallas import tpu as pltpu
from jax.sharding import PartitionSpec as P

HEAD_DIM = 128


norm_eps = 1e-05
rope_base = 500000.0


def from_behind(block, axis, distance):
    devices = range(lax.axis_size(axis))
    route = [((i - distance) % len(devices), i) for i in devices]
    return lax.ppermute(block, axis, route)


def rotate(matrix, positions):
    half_dim = matrix.shape[-1] // 2
    frequency = rope_base ** (-2.0 * jnp.arange(half_dim, dtype=jnp.float32) / matrix.shape[-1])
    angles = positions.astype(jnp.float32)[:, None] * frequency[None, :]
    cos_table = jnp.cos(angles)[:, None, :]
    sin_table = jnp.sin(angles)[:, None, :]
    leading = matrix[..., :half_dim]
    trailing = matrix[..., half_dim:]
    return jnp.concatenate(
        [leading * cos_table - trailing * sin_table, trailing * cos_table + leading * sin_table],
        axis=-1,
    )


def project(tokens, gain, query_matrix, keyval_matrix, positions):
    widened = tokens.astype(jnp.float32)
    inverse = lax.rsqrt(jnp.mean(widened * widened, axis=-1, keepdims=True) + norm_eps)
    normed = (widened * inverse * gain[None, :]).astype(jnp.bfloat16)
    row_count = tokens.shape[0]
    query_full = jnp.dot(normed, query_matrix, preferred_element_type=jnp.float32)
    keyval_full = jnp.dot(normed, keyval_matrix, preferred_element_type=jnp.float32)
    queries = rotate(query_full.reshape(row_count, -1, HEAD_DIM), positions).astype(jnp.bfloat16)
    paired = keyval_full.reshape(row_count, 2, -1, HEAD_DIM)
    key_rows = rotate(paired[:, 0], positions).astype(jnp.bfloat16)
    value_rows = paired[:, 1].astype(jnp.bfloat16)
    return (queries, key_rows, value_rows)


def attend(queries, key_wide, value_wide, query_pos, key_pos, narrow):
    row_count = queries.shape[0]
    kv_count = key_wide.shape[1]
    head_size = queries.shape[2]
    group_size = queries.shape[1] // kv_count
    grouped = jnp.moveaxis(queries.reshape(row_count, kv_count, group_size, head_size), 1, 0)
    key_heads = jnp.moveaxis(key_wide, 1, 0)
    value_heads = jnp.moveaxis(value_wide, 1, 0)
    visible = (key_pos[None, :] <= query_pos[:, None])[None]

    def one_head(block):
        query_block, key_block, value_block = block
        scores = jnp.einsum(
            "rgd,sd->grs", query_block, key_block, preferred_element_type=jnp.float32
        ) * head_size ** (-0.5)
        masked = jnp.where(visible, scores, -1e30)
        row_max = lax.stop_gradient(jnp.max(masked, axis=-1, keepdims=True))
        numerators = jnp.where(visible, jnp.exp(masked - row_max), 0.0)
        totals = jnp.sum(numerators, axis=-1)
        if narrow:
            rounded = numerators.astype(jnp.bfloat16)
        else:
            rounded = lax.optimization_barrier(numerators.astype(jnp.bfloat16)).astype(jnp.float32)
        summed = jnp.einsum("grs,sd->rgd", rounded, value_block, preferred_element_type=jnp.float32)
        return summed / jnp.transpose(totals, (1, 0))[..., None]

    averaged = lax.map(one_head, (grouped, key_heads, value_heads))
    return jnp.moveaxis(averaged, 0, 1).reshape(row_count, -1).astype(jnp.bfloat16)


def finish(tokens, mixed, output_matrix):
    return (
        tokens.astype(jnp.float32)
        + jnp.dot(mixed, output_matrix, preferred_element_type=jnp.float32)
    ).astype(jnp.bfloat16)


def shards(
    section_inputs,
    saved_inputs,
    output_grads,
    token_positions,
    norm_gain,
    query_weight,
    keyval_weight,
    output_weight,
):
    key_positions = lax.all_gather(token_positions, "ctx", axis=0, tiled=True)
    full_query, full_keyval = (
        lax.all_gather(query_weight[0], "ctx", axis=0, tiled=True),
        lax.all_gather(keyval_weight[0], "ctx", axis=0, tiled=True),
    )
    full_output = output_weight[0]
    gain = norm_gain[0]
    forward_tokens = section_inputs[0]
    saved_tokens = saved_inputs[0]
    upstream = output_grads[0]

    def projector(tokens):
        return project(tokens, gain, full_query, full_keyval, token_positions)

    def attention_wide(queries, key_wide, value_wide):
        return attend(queries, key_wide, value_wide, token_positions, key_positions, False)

    def finishing(tokens, mixed):
        return finish(tokens, mixed, full_output)

    forward_queries, forward_keys, forward_values = projector(forward_tokens)
    (backward_queries, backward_keys, backward_values), back_project = jax.vjp(
        projector, saved_tokens
    )
    forward_keyset, forward_valueset = (
        lax.all_gather(forward_keys, "ctx", axis=0, tiled=True),
        lax.all_gather(forward_values, "ctx", axis=0, tiled=True),
    )
    mixed = attend(
        forward_queries, forward_keyset, forward_valueset, token_positions, key_positions, True
    )
    produced = finishing(forward_tokens, mixed)
    sent_on = from_behind(produced[None], "section", 1)
    backward_keyset, backward_valueset = (
        lax.all_gather(backward_keys, "ctx", axis=0, tiled=True),
        lax.all_gather(backward_values, "ctx", axis=0, tiled=True),
    )
    mixed, back_attend = jax.vjp(
        attention_wide,
        backward_queries.astype(jnp.float32),
        backward_keyset.astype(jnp.float32),
        backward_valueset.astype(jnp.float32),
    )
    produced, back_finish = jax.vjp(finishing, saved_tokens, mixed)
    residual_grad, mixed_grad = back_finish(upstream)
    query_grad, key_partial, value_partial = back_attend(mixed_grad)
    key_grads = lax.psum_scatter(
        key_partial.astype(jnp.bfloat16), "ctx", scatter_dimension=0, tiled=True
    )
    value_grads = lax.psum_scatter(
        value_partial.astype(jnp.bfloat16), "ctx", scatter_dimension=0, tiled=True
    )
    (project_grad,) = back_project((query_grad.astype(jnp.bfloat16), key_grads, value_grads))
    sent_back = from_behind((residual_grad + project_grad)[None], "section", -1)
    return (sent_on, sent_back)


MESH = pl.DeviceIdType.MESH
VMEM = pl.BlockSpec(memory_space=pltpu.VMEM)
ANY = pl.BlockSpec(memory_space=pl.ANY)
WIDE = jnp.float32
SLIM = jnp.bfloat16


def remote(src, dst, send, recv, device):
    return pltpu.make_async_remote_copy(
        src_ref=src, dst_ref=dst, send_sem=send, recv_sem=recv, device_id=device, device_id_type=MESH
    )


def layer_kernel(
    n, sections, nf, nb, up, wo_hbm, wq, wkv, pos, waves, tokens, saved, gain, ahead, back,
    xf, xb, mgl, mg, wo, wh, posg, qcol, cos, sin, qkv_f, qkv_b, mixed, dqkv, mixed_in, part, inbox,
    produced, grads, fsend, frecv, gsend, grecv, wsend, wrecv, msend, mrecv, psend, precv,
    asend, arecv, bsend, brecv, csend, crecv, own,
):
    section = lax.axis_index("section")
    me = lax.axis_index("ctx")
    depth, _ = wq.shape
    rows, gq = mg.shape[1:]
    wide = wh.shape[2]
    kvw = (wide - gq) // 2
    half = kvw * n
    group = gq // kvw
    scale = HEAD_DIM ** (-0.5)
    following, preceding = lax.rem(section + 1, sections), lax.rem(section + sections - 1, sections)

    barrier = pltpu.get_barrier_semaphore()
    for k in range(1, n):
        pl.semaphore_signal(barrier, inc=1, device_id=(section, lax.rem(me + k, n)), device_id_type=MESH)
    for other in (following, preceding):
        pl.semaphore_signal(barrier, inc=1, device_id=(other, me), device_id_type=MESH)
    pl.semaphore_wait(barrier, n + 1)

    def peer(side, t):
        return (me + t, me + t < n) if side == 0 else (me - t, me - t >= 0)

    def behind(side, t):
        return peer(1 - side, t)

    def begin(copies):
        for copy in copies:
            copy.start()

    def arrive(copies):
        for copy in copies:
            copy.wait_recv()

    def leave(copies):
        for copy in copies:
            copy.wait_send()

    def weight_copies(side, t, target, source):
        parts = (
            (wq, target * gq, gq, 0),
            (wkv, target * kvw, kvw, gq),
            (wkv, half + target * kvw, kvw, gq + kvw),
        )
        return [
            remote(
                ref.at[:, pl.ds(pl.multiple_of(start, 128), size)],
                wh.at[source, :, pl.ds(to, size)],
                wsend.at[side, t, i], wrecv.at[side, t, i], (section, target),
            )
            for i, (ref, start, size, to) in enumerate(parts)
        ]

    relays = ((nf, xf, fsend, frecv), (nb, xb, gsend, grecv))

    def row_copies(batch, side, t, block, target):
        first, every, send, recv = relays[batch]
        return [
            remote(
                first if t == 1 else every.at[block], every.at[block],
                send.at[side, t], recv.at[side, t], (section, target),
            )
        ]

    def small_copies(side, t, target):
        return [remote(mgl.at[target], mg.at[me], msend.at[side, t], mrecv.at[side, t], (section, target))]

    def place_copies(side, t, target):
        return [remote(pos, posg.at[me], psend.at[side, t], precv.at[side, t], (section, target))]

    def mixed_copies(side, t, target):
        return [
            remote(mixed.at[target], mixed_in.at[me], asend.at[side, t], arecv.at[side, t], (section, target))
        ]

    def hop(batch, side, t):
        block, there = behind(side, t)
        target, fits = peer(side, 1)
        pl.when(there)(lambda: arrive(row_copies(batch, side, t, block, me)))
        if t + 1 < n:
            pl.when(jnp.logical_and(there, fits))(
                lambda: begin(row_copies(batch, side, t + 1, block, target))
            )

    def send_own(batch):
        for side in (0, 1):
            target, fits = peer(side, 1)
            pl.when(fits)(lambda: begin(row_copies(batch, side, 1, me, target)))

    def to_all(copies, action):
        for t in range(n - 1, 0, -1):
            for side in (0, 1):
                target, fits = peer(side, t)
                pl.when(fits)(lambda: action(copies(side, t, target)))

    def from_all(copies):
        for t in range(1, n):
            for side in (0, 1):
                _, there = behind(side, t)
                pl.when(there)(lambda: arrive(copies(side, t, me)))

    send_own(0)
    send_own(1)
    to_all(place_copies, begin)
    wo_copy = pltpu.make_async_copy(wo_hbm, wo, own.at[0])
    wo_copy.start()
    mine = [
        pltpu.make_async_copy(
            ref.at[:, pl.ds(pl.multiple_of(start, 128), size)], wh.at[me, :, pl.ds(to, size)], own.at[i + 1]
        )
        for i, (ref, start, size, to) in enumerate(
            ((wq, me * gq, gq, 0), (wkv, me * kvw, kvw, gq), (wkv, half + me * kvw, kvw, gq + kvw))
        )
    ]
    begin(mine)
    posg[me] = pos[...]
    xf[me] = nf[...]
    xb[me] = nb[...]

    def send_weights(side):
        for t in range(n - 1, 0, -1):
            target, fits = peer(side, t)
            pl.when(fits)(lambda: begin(weight_copies(side, t, target, me)))

    for t in range(1, n):
        pl.when(me == t - 1)(lambda: send_weights(0))
        pl.when(n - me == t)(lambda: send_weights(1))
        for batch in (0, 1):
            for side in (0, 1):
                hop(batch, side, t)

    wo_copy.wait()
    for j in range(n):
        mgl[j] = lax.dot_general(
            up[...], wo[pl.ds(j * gq, gq), :], (((1,), (1,)), ((), ())), preferred_element_type=WIDE
        ).astype(SLIM)
    mg[me] = mgl[me]
    to_all(small_copies, begin)

    from_all(place_copies)
    for j in range(n):
        column = jnp.transpose(jnp.broadcast_to(posg[j].astype(WIDE), (HEAD_DIM, rows)))
        angles = column * waves[0:1, :]
        qcol[j] = column
        cos[pl.ds(j * rows, rows), :] = jnp.cos(angles)
        sin[pl.ds(j * rows, rows), :] = jnp.sin(angles) * waves[1:2, :]

    tile = 256 if wide % 256 == 0 else 128

    def add_from(j, first):
        columns = pl.ds(pl.multiple_of(j * depth, 128), depth)

        @pl.loop(0, wide // tile)
        def _(c):
            at = pl.ds(pl.multiple_of(c * tile, 128), tile)
            for every, total in ((xf, qkv_f), (xb, qkv_b)):
                term = jnp.dot(
                    every[:, :, columns].reshape(-1, depth), wh[j, :, at], preferred_element_type=WIDE
                )
                total[:, at] = term if first else total[:, at] + term

    for copy in mine:
        copy.wait()
    add_from(me, True)
    for t in range(1, n):
        for side in (0, 1):
            block, there = behind(side, t)

            @pl.when(there)
            def _():
                arrive(weight_copies(side, t, me, block))
                add_from(block, False)

    column = qcol[...].reshape(n * rows, HEAD_DIM)
    visible = jnp.transpose(column)[0:1, :] <= column[:, 0:1]

    def turn(block, sign):
        return block * cos[...] + sign * (pltpu.roll(block, HEAD_DIM // 2, 1) * sin[...])

    def dot(a, b, dims):
        return lax.dot_general(a, b, (dims, ((), ())), preferred_element_type=WIDE)

    def weigh(queries, keys):
        scores = dot(queries, keys, ((1,), (1,))) * scale
        masked = jnp.where(visible, scores, -1e30)
        row_max = jnp.max(masked, axis=-1, keepdims=True)
        numerators = jnp.where(visible, jnp.exp(masked - row_max), 0.0)
        return numerators, jnp.sum(numerators, axis=-1, keepdims=True)

    def head_at(kv, h):
        return pl.ds(pl.multiple_of((kv * group + h) * HEAD_DIM, HEAD_DIM), HEAD_DIM)

    def keys_and_values(qkv, kv):
        keys = turn(qkv[:, pl.ds(gq + kv * HEAD_DIM, HEAD_DIM)], 1.0).astype(SLIM)
        return keys, qkv[:, pl.ds(gq + kvw + kv * HEAD_DIM, HEAD_DIM)].astype(SLIM)

    for kv in range(kvw // HEAD_DIM):
        keys, values = keys_and_values(qkv_f, kv)

        @pl.loop(0, group)
        def _(h):
            at = head_at(kv, h)
            numerators, totals = weigh(turn(qkv_f[:, at], 1.0).astype(SLIM), keys)
            result = dot(numerators.astype(SLIM), values, ((1,), (0,))) / totals
            mixed[:, :, at] = result.astype(SLIM).reshape(n, rows, HEAD_DIM)

    to_all(mixed_copies, begin)

    from_all(small_copies)
    for kv in range(kvw // HEAD_DIM):
        keys, values = keys_and_values(qkv_b, kv)

        def head(h, sums):
            at = head_at(kv, h)
            queries = turn(qkv_b[:, at], 1.0).astype(SLIM)
            numerators, totals = weigh(queries, keys)
            rounded = numerators.astype(SLIM)
            summed = dot(rounded, values, ((1,), (0,)))
            summed_grad = mg[:, :, at].reshape(n * rows, HEAD_DIM).astype(WIDE) / totals
            totals_grad = -jnp.sum(summed_grad * (summed / totals), axis=-1, keepdims=True)
            narrow_grad = summed_grad.astype(SLIM)
            numer_grad = dot(narrow_grad, values, ((1,), (1,))) + totals_grad
            score_grad = (numerators * numer_grad * scale).astype(SLIM)
            query_grad = dot(score_grad, keys, ((1,), (0,))).astype(SLIM)
            dqkv[:, at] = turn(query_grad.astype(WIDE), -1.0).astype(SLIM)
            key_grad, value_grad = sums
            return (
                key_grad + dot(score_grad, queries, ((0,), (0,))),
                value_grad + dot(rounded, narrow_grad, ((0,), (0,))),
            )

        nothing = jnp.zeros(keys.shape, WIDE)
        key_grad, value_grad = lax.fori_loop(0, group, head, (nothing, nothing))
        dqkv[:, pl.ds(gq + kv * HEAD_DIM, HEAD_DIM)] = turn(
            key_grad.astype(SLIM).astype(WIDE), -1.0
        ).astype(SLIM)
        dqkv[:, pl.ds(gq + kvw + kv * HEAD_DIM, HEAD_DIM)] = value_grad.astype(SLIM)

    def sum_copy(side, r, block, target):
        return remote(
            part.at[block], inbox.at[side, r - 1], bsend.at[side, r], brecv.at[side, r - 1], (section, target)
        )

    def partial_grad(block, sides_in, r):
        mine_rows = dqkv[pl.ds(pl.multiple_of(block * rows, 16), rows), :]
        for j in range(n):
            part[block, :, pl.ds(j * depth, depth)] = lax.dot_general(
                mine_rows, wh[j], (((1,), (1,)), ((), ())), preferred_element_type=WIDE
            ).astype(SLIM)
        for side in sides_in:
            _, there = behind(side, 1)

            @pl.when(there)
            def _():
                sum_copy(side, r + 1, block, me).wait_recv()
                part[block] = (part[block].astype(WIDE) + inbox[side, r].astype(WIDE)).astype(SLIM)

    def sum_step(r):
        for side in (0, 1):
            block, there = peer(side, r)
            target, _ = peer(side, 1)

            @pl.when(there)
            def _():
                partial_grad(block, (side,), r)
                sum_copy(side, r, block, target).start()

    sum_step(n - 1)
    total = tokens[...].astype(WIDE)
    total += jnp.dot(
        mixed[me], wo[pl.ds(pl.multiple_of(me * gq, 128), gq), :], preferred_element_type=WIDE
    )
    from_all(mixed_copies)
    for k in range(1, n):
        source = lax.rem(me + k, n)
        at = pl.ds(pl.multiple_of(source * gq, 128), gq)
        total += jnp.dot(mixed_in[source], wo[at, :], preferred_element_type=WIDE)
    produced[...] = total.astype(SLIM)
    ahead_copy = remote(produced, ahead, csend.at[0], crecv.at[0], (following, me))
    ahead_copy.start()
    for r in range(n - 2, 0, -1):
        sum_step(r)
    partial_grad(me, (0, 1), 0)

    widened = saved[...].astype(WIDE)
    inverse = lax.rsqrt(jnp.mean(widened * widened, axis=-1, keepdims=True) + norm_eps)
    scaled = part[me].astype(WIDE) * gain[...]
    inner = jnp.mean(scaled * widened, axis=-1, keepdims=True)
    project_grad = inverse * scaled - widened * (inverse * inverse * inverse * inner)
    grads[...] = up[...] + project_grad.astype(SLIM)
    back_copy = remote(grads, back, csend.at[1], crecv.at[1], (preceding, me))
    back_copy.start()

    to_all(lambda side, t, target: weight_copies(side, t, target, me), leave)
    for copies in (small_copies, place_copies, mixed_copies):
        to_all(copies, leave)
    for t in range(1, n):
        for side in (0, 1):
            block, there = behind(side, t - 1)
            target, fits = peer(side, 1)

            @pl.when(jnp.logical_and(there, fits))
            def _():
                for batch in (0, 1):
                    leave(row_copies(batch, side, t, block, target))

            block, there = peer(side, t)
            pl.when(there)(lambda: leave([sum_copy(side, t, block, target)]))
    ahead_copy.wait()
    back_copy.wait()


def norm_kernel(first, second, gain, first_out, second_out):
    for tokens, normed in ((first, first_out), (second, second_out)):
        widened = tokens[...].astype(WIDE)
        inverse = lax.rsqrt(jnp.mean(widened * widened, axis=-1, keepdims=True) + norm_eps)
        normed[...] = (widened * inverse * gain[...]).astype(SLIM)


def hand_kernel(first, second, first_out, second_out):
    first_out[...] = first[...]
    second_out[...] = second[...]


def by_heads(n, sections):
    def step(
        section_inputs, saved_inputs, output_grads, token_positions, norm_gain,
        query_weight, keyval_weight, output_weight,
    ):
        _, rows, width = section_inputs.shape
        _, depth, query_width = query_weight.shape
        gq = query_width // n
        wide = gq + keyval_weight.shape[2] // n

        half_dim = HEAD_DIM // 2
        frequency = rope_base ** (-2.0 * np.arange(half_dim) / HEAD_DIM)
        signs = np.ones(half_dim)
        waves = jnp.asarray(
            np.stack([np.concatenate([frequency, frequency]), np.concatenate([-signs, signs])]), WIDE
        )

        def shaped(shape, kind=SLIM):
            return jax.ShapeDtypeStruct(shape, kind)

        def held(*shape, kind=SLIM):
            return pltpu.VMEM(shape, kind)

        pair = (shaped((rows, width)), shaped((rows, width)))
        normed_f, normed_b = pl.pallas_call(
            norm_kernel, out_shape=pair, in_specs=[VMEM] * 3, out_specs=(VMEM,) * 2, name="norm"
        )(section_inputs[0], saved_inputs[0], norm_gain)
        dma = pltpu.SemaphoreType.DMA
        ahead, back = pl.pallas_call(
            functools.partial(layer_kernel, n, sections),
            out_shape=pair,
            in_specs=[VMEM, VMEM, VMEM, ANY, ANY, ANY, VMEM, VMEM, VMEM, VMEM, VMEM],
            out_specs=(VMEM,) * 2,
            scratch_shapes=[
                held(n, rows, width), held(n, rows, width),
                held(n, rows, gq), held(n, rows, gq), held(query_width, width), held(n, depth, wide),
                held(n, 1, rows, kind=jnp.int32), held(n, rows, HEAD_DIM, kind=WIDE),
                held(n * rows, HEAD_DIM, kind=WIDE), held(n * rows, HEAD_DIM, kind=WIDE),
                held(n * rows, wide, kind=WIDE), held(n * rows, wide, kind=WIDE),
                held(n, rows, gq), held(n * rows, wide), held(n, rows, gq),
                held(n, rows, width), held(2, n, rows, width),
                held(rows, width), held(rows, width),
                *[dma((2, n))] * 4, *[dma((2, n, 3))] * 2, *[dma((2, n))] * 8, *[dma((2,))] * 2, dma((4,)),
            ],
            compiler_params=pltpu.CompilerParams(
                collective_id=0, has_side_effects=True, vmem_limit_bytes=60 * 2**20
            ),
            name="layer",
        )(
            normed_f, normed_b, output_grads[0], output_weight[0],
            query_weight[0], keyval_weight[0], token_positions[None], waves,
            section_inputs[0], saved_inputs[0], norm_gain,
        )
        ahead, back = pl.pallas_call(
            hand_kernel, out_shape=pair, in_specs=[VMEM] * 2, out_specs=(VMEM,) * 2, name="hand"
        )(ahead, back)
        return (ahead[None], back[None])

    return step


def solution(mesh):
    placed = (
        P("section", "ctx", None),
        P("section", "ctx", None),
        P("section", "ctx", None),
        P("ctx"),
        P("section", None),
        P("section", "ctx", None),
        P("section", "ctx", None),
        P("section", None, None),
    )
    n, sections = mesh.shape["ctx"], mesh.shape["section"]

    def chosen(*blocks):
        kv_heads = blocks[6].shape[2] // (2 * HEAD_DIM)
        if n > 1 and sections > 2 and kv_heads % n == 0:
            return by_heads(n, sections)(*blocks)
        return shards(*blocks)

    return jax.shard_map(
        chosen,
        mesh=mesh,
        in_specs=placed,
        out_specs=(P("section", "ctx", None), P("section", "ctx", None)),
        check_vma=False,
    )
```
